32 devices in a mesh: row: 4 (over y, x), blk: 8 (over z, core).
Axes of the slice: x: 2, y: 2, z: 4, core: 2. Of those that a mesh axis runs over, the one named last changes fastest.
Arguments:
- elastic_kernel: bfloat16 [8, 512, 4, 1024], P('blk', None, 'row'), may hold values from -0.125 to 0.125
- slip_deficit: float32 [8, 4, 128, 512], P('blk', 'row'), may hold values from -6 to 6
- state_variable: float32 [8, 4, 128, 512], P('blk', 'row'), may hold values from 0.2 to 5
- step_size: float32 [512], replicated, may hold values from 0.02 to 0.1
- load_stress: float32 [8, 4, 128], P('blk', 'row'), may hold values from -6 to 6
- normal_stress: float32 [8, 4, 128], P('blk', 'row'), may hold values from 0.5 to 2
- rate_table: float32 [16], replicated, may hold values from 0.3 to 1
- evolve_table: float32 [16], replicated, may hold values from 0.3 to 1.5
- patch_region: int32 [8, 4, 128], P('blk', 'row'), may hold values from 0 to 15
- creep_flag: int32 [8, 4, 128], P('blk', 'row'), may hold values 0 or 1
Outputs:
- velocity: float32 [8, 4, 128, 512], P('blk', 'row')
- deficit_out: float32 [8, 4, 128, 512], P('blk', 'row')
- state_out: float32 [8, 4, 128, 512], P('blk', 'row')
- step_next: float32 [512], replicated
The draws below stay inside these ranges and needn't reach their ends.
All inputs are finite; a program needn't handle non-finite values. Where the reference program divides by a largest or mean magnitude, that divisor is 1e-20 or more. No bound on the sum of `creep_flag` on one device may be relied on, other than what follows from the above.
Results may differ from the reference program's by a relative error of at most 0.0035.
Values may be sent and summed in bfloat16 or wider, within the bound.
A program may use at most 64 MiB of HBM per device.

```python
import math
import jax
import jax.numpy as jnp
from jax import lax

ELEM_DEV = 128
MEMBERS = 512
REGIONS = 16
NEWTON = 3
STEPS = 2
ROW_GROUPS = 4
COL_BLOCKS = 8
ELEMENTS = 4096


def touch_ends(array, own_key, least, high):
    longest = array.shape.index(max(array.shape))
    spots = []
    for shift in (0, 1):
        where = [jax.random.randint(jax.random.fold_in(own_key, axis), (), 0, length) for axis, length in enumerate(array.shape)]
        where[longest] = (where[longest] + shift) % array.shape[longest]
        spots.append(tuple(where))
    return array.at[spots[0]].set(least).at[spots[1]].set(high)


def strengthened(array, key, source, target, blocks, factor):
    def block_of(dim):
        return (jnp.arange(array.shape[dim]) // (array.shape[dim] // blocks)).reshape((-1,) + (1,) * (array.ndim - 1 - dim))

    near = jax.random.permutation(key, blocks)[block_of(target)]
    far = (block_of(target) + blocks // 2) % blocks
    return jnp.where((block_of(source) == near) | (block_of(source) == far), factor * array, array)


def steps_of(own_key, extent, shards, least, top_value):
    def one(position, blocks):
        steps = jax.random.uniform(jax.random.fold_in(jax.random.fold_in(own_key, 6), position), (blocks,), jnp.float32, least / len(shards), top_value / len(shards))
        return jnp.repeat(jnp.exp(steps), extent[position] // blocks).reshape((-1,) + (1,) * (len(extent) - position - 1))

    gain = one(*shards[0])
    for cut in shards[1:]:
        gain = gain * one(*cut)
    return gain


def gaussian(rng, shape, width, reach, pieces=(), kind=jnp.bfloat16):
    values = jax.random.normal(rng, shape, jnp.float32) * width
    if len(pieces) > 0:
        values = steps_of(rng, shape, pieces, -0.22, 0.18) * values
    return jnp.clip(values, min=-reach, max=reach).astype(kind)


def bell_draw_with(rng, shape, spread, reach, shards, heavy, held_as=jnp.bfloat16):
    values = spread * jax.random.normal(rng, shape, jnp.float32)
    if shards:
        values = values * steps_of(rng, shape, shards, -0.22, 0.18)
    return jnp.clip(strengthened(values, jax.random.fold_in(rng, 3), *heavy), -reach, reach).astype(held_as)


def setup_inputs(seed: int = 0) -> dict:
    splits = jax.random.split(jax.random.key(seed), 11)
    elastic_kernel = bell_draw_with(splits[0], (COL_BLOCKS, ROW_GROUPS * ELEM_DEV, ROW_GROUPS, COL_BLOCKS * ELEM_DEV), ELEMENTS ** -0.5, 0.125, ((0, 8), (2, 4)), (2, 1, 4, 2.0))
    slip_deficit = gaussian(splits[1], (COL_BLOCKS, ROW_GROUPS, ELEM_DEV, MEMBERS), 1.0, 6.0, ((0, 8), (1, 4)), jnp.float32)
    state_variable = jnp.clip(jnp.exp(math.log(5.0) - 3.218876 * jax.random.uniform(splits[2], (COL_BLOCKS, ROW_GROUPS, ELEM_DEV, MEMBERS), jnp.float32) ** steps_of(splits[2], (COL_BLOCKS, ROW_GROUPS, ELEM_DEV, MEMBERS), ((0, 8), (1, 4)), -0.2, 0.2)), 0.2, 5.0)
    step_size = jnp.clip(jnp.exp(jax.random.uniform(splits[3], (MEMBERS,), jnp.float32, math.log(0.02), math.log(0.1))), 0.02, 0.1)
    load_stress = gaussian(splits[4], (COL_BLOCKS, ROW_GROUPS, ELEM_DEV), 1.0, 6.0, ((0, 8), (1, 4)), jnp.float32)
    normal_stress = jnp.clip(jnp.exp(math.log(2.0) - 1.3862944 * jax.random.uniform(splits[5], (COL_BLOCKS, ROW_GROUPS, ELEM_DEV), jnp.float32) ** steps_of(splits[5], (COL_BLOCKS, ROW_GROUPS, ELEM_DEV), ((0, 8), (1, 4)), -0.2, 0.2)), 0.5, 2.0)
    rate_table = jnp.clip(jnp.exp(jax.random.uniform(splits[6], (REGIONS,), jnp.float32, math.log(0.3), math.log(1.0))), 0.3, 1.0)
    evolve_table = jnp.clip(jnp.exp(jax.random.uniform(splits[7], (REGIONS,), jnp.float32, math.log(0.3), math.log(1.5))), 0.3, 1.5)
    patch_region = touch_ends(jax.random.randint(splits[8], (COL_BLOCKS, ROW_GROUPS, ELEM_DEV), 0, REGIONS), jax.random.fold_in(splits[8], 1), 0, REGIONS - 1).astype(jnp.int32)
    creep_flag = touch_ends((jax.random.randint(splits[9], (COL_BLOCKS, ROW_GROUPS, ELEM_DEV), 0, 4) < 1).astype(jnp.int32), jax.random.fold_in(splits[9], 1), 0, 1)
    return {"elastic_kernel": elastic_kernel, "slip_deficit": slip_deficit, "state_variable": state_variable, "step_size": step_size, "load_stress": load_stress, "normal_stress": normal_stress, "rate_table": rate_table, "evolve_table": evolve_table, "patch_region": patch_region, "creep_flag": creep_flag}


DAMPING = 0.5
PLATE_RATE = 1.0
STEP_CAP = 0.5

def inverse_sinh(value):
    magnitude = jnp.abs(value)
    result = jnp.log(magnitude + jnp.sqrt(magnitude * magnitude + 1.0))
    return jnp.where(value < 0.0, -result, result)

def tractions(elastic_kernel, deficit):
    slip = deficit.astype(jnp.bfloat16)
    sources = jnp.transpose(slip, (1, 0, 2, 3)).reshape(-1, slip.shape[3])

    def one_block(kernel_block):
        flat = kernel_block.reshape(kernel_block.shape[0], -1)
        return jnp.dot(flat, sources, preferred_element_type=jnp.float32)
    result = lax.map(one_block, elastic_kernel)
    return result.reshape(slip.shape)

def solve_rate(stress, pressure, rate_coef, state_coef, state, creeping):
    factor = 0.5 * jnp.exp(state_coef * jnp.log(state) / rate_coef)
    strength = pressure * rate_coef
    speed = stress / (strength * factor + DAMPING)
    for repeat in range(NEWTON):
        scaled = factor * speed
        mismatch = strength * inverse_sinh(scaled) + DAMPING * speed - stress
        gradient = strength * factor / jnp.sqrt(1.0 + scaled * scaled) + DAMPING
        speed = speed - mismatch / gradient
    return jnp.where(creeping, jnp.float32(PLATE_RATE), speed)

def reference(elastic_kernel, slip_deficit, state_variable, step_size, load_stress, normal_stress, rate_table, evolve_table, patch_region, creep_flag):
    levels = jnp.arange(rate_table.shape[0], dtype=jnp.int32)
    onehot = (patch_region[..., None] == levels).astype(jnp.float32)
    rate_coef = lax.optimization_barrier(jnp.sum(onehot * rate_table, axis=-1))[..., None]
    state_coef = lax.optimization_barrier(jnp.sum(onehot * evolve_table, axis=-1))[..., None]
    pressure = normal_stress[..., None]
    loading = load_stress[..., None]
    creeping = (creep_flag == 1)[..., None]
    deficit = slip_deficit
    state = state_variable
    step_now = step_size
    velocity = jnp.zeros_like(deficit)
    for repeat in range(STEPS):
        stress = loading + tractions(elastic_kernel, deficit)
        velocity = solve_rate(stress, pressure, rate_coef, state_coef, state, creeping)
        largest = lax.optimization_barrier(jnp.max(jnp.abs(velocity), axis=(0, 1, 2)))
        state = state * jnp.exp(step_now * (1.0 / state - jnp.abs(velocity)))
        deficit = deficit + step_now * (velocity - PLATE_RATE)
        step_now = STEP_CAP / (1.0 + largest)
    return (velocity, deficit, state, step_now)
```

```python
import functools

import jax
import jax.numpy as jnp
from jax import lax
from jax.experimental import pallas as pl
from jax.experimental.pallas import tpu as pltpu
from jax.sharding import PartitionSpec as P

NEWTON = 3
STEPS = 2
CORES = 2
CHUNK = 128

DAMPING = 0.5
PLATE_RATE = 1.0
STEP_CAP = 0.5

MESH = pl.DeviceIdType.MESH


def solve_rate(stress, factor, strength, creeping):
    slope = strength * factor
    speed = stress / (slope + DAMPING)
    for repeat in range(NEWTON):
        scaled = factor * speed
        size = jnp.abs(scaled)
        root = jnp.sqrt(size * size + 1.0)
        bend = jnp.log(size + root)
        bend = jnp.where(scaled < 0.0, -bend, bend)
        mismatch = strength * bend + DAMPING * speed - stress
        gradient = slope / root + DAMPING
        speed = speed - mismatch / gradient
    return jnp.where(creeping, jnp.float32(PLATE_RATE), speed)


def fault_kernel(
    rows,
    blks,
    chunks,
    elastic_in,
    deficit_in,
    state_in,
    step_ref,
    load_ref,
    normal_ref,
    rate_ref,
    evolve_ref,
    region_ref,
    creep_ref,
    velocity_out,
    deficit_out,
    state_out,
    next_out,
    tile,
    deficit,
    state,
    velocity,
    gathered,
    parts,
    own,
    partial,
    received,
    coefs,
    max_one,
    max_row,
    max_two,
    max_blk,
    load_sems,
    out_sems,
    own_sems,
    relay_sems,
    slip_sems,
    sum_send,
    sum_recv,
    row_send,
    row_recv,
    blk_send,
    blk_recv,
):
    me_row = lax.axis_index("row")
    me_blk = lax.axis_index("blk")
    spots = blks // CORES
    spot = me_blk // CORES
    core = me_blk % CORES
    elements, width = deficit.shape[1:]
    half = elements // 2
    sent = []

    def columns(c):
        return pl.ds(c * width, width)

    def remote(src, dst, send_sem, recv_sem, row, blk):
        return pltpu.make_async_remote_copy(
            src_ref=src,
            dst_ref=dst,
            send_sem=send_sem,
            recv_sem=recv_sem,
            device_id={"row": row, "blk": blk},
            device_id_type=MESH,
        )

    def launch(copy, when=None):
        if when is None:
            copy.start()
        else:
            pl.when(when)(copy.start)
        sent.append((copy, when))

    deficit_loads = [
        pltpu.make_async_copy(deficit_in.at[:, columns(c)], deficit.at[c], load_sems.at[0, c])
        for c in range(chunks)
    ]
    state_loads = [
        pltpu.make_async_copy(state_in.at[:, columns(c)], state.at[c], load_sems.at[1, c])
        for c in range(chunks)
    ]
    tile_load = pltpu.make_async_copy(elastic_in, tile, load_sems.at[2, 0])
    for copy in deficit_loads + state_loads + [tile_load]:
        copy.start()

    barrier = pltpu.get_barrier_semaphore()
    for j in range(1, rows):
        pl.semaphore_signal(
            barrier,
            inc=1,
            device_id={"row": lax.rem(me_row + j, rows), "blk": me_blk},
            device_id_type=MESH,
        )
    for j in range(1, blks):
        pl.semaphore_signal(
            barrier,
            inc=1,
            device_id={"row": me_row, "blk": lax.rem(me_blk + j, blks)},
            device_id_type=MESH,
        )
    for c in range(chunks):
        deficit_loads[c].wait()
        gathered[0, c, me_blk] = deficit[c].astype(jnp.bfloat16)
    pl.semaphore_wait(barrier, rows + blks - 2)

    def slip_copy(t, c, block, target, sem):
        place = gathered.at[t, c, block]
        return remote(place, place, sem, slip_sems.at[t, c, block], me_row, target)

    def partner_copy(t, c, block, sem):
        return slip_copy(t, c, block, spot * CORES + 1 - core, sem)

    def send_own(t, c):
        for i, shift in enumerate((2, -2, 1, -1)):
            target = spot + shift
            launch(
                slip_copy(t, c, me_blk, target * CORES + core, own_sems.at[t, c, i]),
                (target >= 0) & (target < spots),
            )
        launch(partner_copy(t, c, me_blk, own_sems.at[t, c, 4]))

    def arrived(t, c, block):
        place = gathered.at[t, c, block]
        pltpu.make_async_copy(place, place, slip_sems.at[t, c, block]).wait()

    def gather(t, c):
        order = [d for d in range(1, spots) if d % 2 == 0]
        order += [d for d in range(1, spots) if d % 2 == 1]
        for d in order:
            for i, side in enumerate((-1, 1)):
                source = spot + side * d
                inside = (source >= 0) & (source < spots)
                block = source * CORES + core
                pl.when(inside)(functools.partial(arrived, t, c, block))
                if d % 2 == 0:
                    for j, shift in enumerate((2, 1)):
                        target = spot - side * shift
                        launch(
                            slip_copy(t, c, block, target * CORES + core, relay_sems.at[t, c, d - 1, i, j]),
                            inside & (target >= 0) & (target < spots),
                        )
                launch(partner_copy(t, c, block, relay_sems.at[t, c, d - 1, i, 2]), inside)
        for s in range(spots):
            arrived(t, c, s * CORES + 1 - core)
        total = jnp.dot(
            tile[...],
            gathered[t, c].reshape(blks * elements, width),
            preferred_element_type=jnp.float32,
        ).reshape(rows, elements, width)
        parts[...] = total
        partial[t, c] = total.astype(jnp.bfloat16)
        for j in range(1, rows):
            target = lax.rem(me_row + j, rows)
            launch(
                remote(
                    partial.at[t, c, target],
                    received.at[t, c, j - 1],
                    sum_send.at[t, c, j - 1],
                    sum_recv.at[t, c, j - 1],
                    target,
                    me_blk,
                )
            )
        own[c] = parts[me_row]

    def landed(place, sem):
        pltpu.make_async_copy(place, place, sem).wait()

    def first_round(t, c, largest):
        max_one[t, c] = largest
        for j in range(1, rows):
            launch(
                remote(
                    max_one.at[t, c],
                    max_row.at[t, c, j - 1],
                    row_send.at[t, c, j - 1],
                    row_recv.at[t, c, j - 1],
                    lax.rem(me_row + j, rows),
                    me_blk,
                )
            )

    def second_round(t, c):
        largest = max_one[t, c]
        for j in range(rows - 1):
            landed(max_row.at[t, c, j], row_recv.at[t, c, j])
            largest = jnp.maximum(largest, max_row[t, c, j])
        max_two[t, c] = largest
        for j in range(1, blks):
            launch(
                remote(
                    max_two.at[t, c],
                    max_blk.at[t, c, j - 1],
                    blk_send.at[t, c, j - 1],
                    blk_recv.at[t, c, j - 1],
                    me_row,
                    lax.rem(me_blk + j, blks),
                )
            )

    def next_step(t, c):
        largest = max_two[t, c]
        for j in range(blks - 1):
            landed(max_blk.at[t, c, j], blk_recv.at[t, c, j])
            largest = jnp.maximum(largest, max_blk[t, c, j])
        return STEP_CAP / (1.0 + largest)

    def friction(t, c):
        for h in range(2):
            part = pl.ds(h * half, half)
            coefs[4 + t, c, part] = 0.5 * jnp.exp(jnp.log(state[c, part]) * coefs[2, 0, part])

    def update(t, c):
        for j in range(rows - 1):
            landed(received.at[t, c, j], sum_recv.at[t, c, j])
        last = t == STEPS - 1
        largest = jnp.zeros((1, width), jnp.float32)
        for h in range(2):
            part = pl.ds(h * half, half)
            stress = coefs[0, 0, part] + own[c, part]
            for j in range(rows - 1):
                stress = stress + received[t, c, j, part].astype(jnp.float32)
            speed = solve_rate(stress, coefs[4 + t, c, part], coefs[1, 0, part], coefs[3, 0, part] > 0.5)
            velocity[c, part] = speed
            largest = jnp.maximum(largest, jnp.max(jnp.abs(speed), axis=0, keepdims=True))
            if not last:
                moved = deficit[c, part] + step_ref[:, columns(c)] * (speed - PLATE_RATE)
                deficit[c, part] = moved
                gathered[t + 1, c, me_blk, part] = moved.astype(jnp.bfloat16)
        if last:
            first_round(t, c, largest)
            velocity_stores[c].start()
            step_now = next_step(t - 1, c)
        else:
            send_own(t + 1, c)
            first_round(t, c, largest)
            step_now = step_ref[:, columns(c)]
        for h in range(2):
            part = pl.ds(h * half, half)
            speed = velocity[c, part]
            old = state[c, part]
            state[c, part] = old * jnp.exp(step_now * (1.0 / old - jnp.abs(speed)))
            if last:
                deficit[c, part] = deficit[c, part] + step_now * (speed - PLATE_RATE)
        if last:
            deficit_stores[c].start()
            state_stores[c].start()
        else:
            friction(t + 1, c)

    velocity_stores, deficit_stores, state_stores = (
        [
            pltpu.make_async_copy(held.at[c], out.at[:, columns(c)], out_sems.at[i, c])
            for c in range(chunks)
        ]
        for i, (held, out) in enumerate(
            ((velocity, velocity_out), (deficit, deficit_out), (state, state_out))
        )
    )

    for c in range(chunks):
        send_own(0, c)

    region = region_ref[...]
    rate_coef = jnp.zeros(region.shape, jnp.float32)
    state_coef = jnp.zeros(region.shape, jnp.float32)
    for level in range(rate_ref.shape[0]):
        match = region == level
        rate_coef = jnp.where(match, rate_ref[level], rate_coef)
        state_coef = jnp.where(match, evolve_ref[level], state_coef)

    def spread(line):
        return jnp.transpose(jnp.broadcast_to(line, (width, elements)))

    coefs[0, 0] = spread(load_ref[...])
    coefs[1, 0] = spread(normal_ref[...] * rate_coef)
    coefs[2, 0] = spread(state_coef / rate_coef)
    coefs[3, 0] = spread(jnp.where(creep_ref[...] == 1, 1.0, 0.0))
    for c in range(chunks):
        state_loads[c].wait()
        friction(0, c)
    tile_load.wait()

    stages = [(t, c) for t in range(STEPS) for c in range(chunks)]
    for s in range(len(stages) + 2):
        if s < len(stages):
            gather(*stages[s])
        if 0 <= s - 1 < len(stages):
            update(*stages[s - 1])
        if 0 <= s - 2:
            second_round(*stages[s - 2])
    for c in range(chunks):
        next_out[:, columns(c)] = next_step(STEPS - 1, c)

    for copy in velocity_stores + deficit_stores + state_stores:
        copy.wait()
    for copy, when in sent:
        if when is None:
            copy.wait_send()
        else:
            pl.when(when)(copy.wait_send)


def shards(
    rows,
    blks,
    elastic_kernel,
    slip_deficit,
    state_variable,
    step_size,
    load_stress,
    normal_stress,
    rate_table,
    evolve_table,
    patch_region,
    creep_flag,
):
    elements, members = slip_deficit.shape[2:]
    width = CHUNK if members % CHUNK == 0 else members
    chunks = members // width
    spots = blks // CORES
    anywhere = pl.BlockSpec(memory_space=pl.ANY)
    vmem = pl.BlockSpec(memory_space=pltpu.VMEM)
    smem = pl.BlockSpec(memory_space=pltpu.SMEM)
    block = jax.ShapeDtypeStruct((elements, members), jnp.float32)
    dma = pltpu.SemaphoreType.DMA
    velocity, deficit, state, step_next = pl.pallas_call(
        functools.partial(fault_kernel, rows, blks, chunks),
        out_shape=(block, block, block, jax.ShapeDtypeStruct((1, members), jnp.float32)),
        in_specs=[anywhere] * 3 + [vmem] * 3 + [smem] * 2 + [vmem] * 2,
        out_specs=(anywhere, anywhere, anywhere, vmem),
        scratch_shapes=[
            pltpu.VMEM((elastic_kernel.shape[1], elastic_kernel.shape[3]), jnp.bfloat16),
            pltpu.VMEM((chunks, elements, width), jnp.float32),
            pltpu.VMEM((chunks, elements, width), jnp.float32),
            pltpu.VMEM((chunks, elements, width), jnp.float32),
            pltpu.VMEM((STEPS, chunks, blks, elements, width), jnp.bfloat16),
            pltpu.VMEM((rows, elements, width), jnp.float32),
            pltpu.VMEM((chunks, elements, width), jnp.float32),
            pltpu.VMEM((STEPS, chunks, rows, elements, width), jnp.bfloat16),
            pltpu.VMEM((STEPS, chunks, rows - 1, elements, width), jnp.bfloat16),
            pltpu.VMEM((4 + STEPS, chunks, elements, width), jnp.float32),
            pltpu.VMEM((STEPS, chunks, 1, width), jnp.float32),
            pltpu.VMEM((STEPS, chunks, rows - 1, 1, width), jnp.float32),
            pltpu.VMEM((STEPS, chunks, 1, width), jnp.float32),
            pltpu.VMEM((STEPS, chunks, blks - 1, 1, width), jnp.float32),
            dma((3, chunks)),
            dma((3, chunks)),
            dma((STEPS, chunks, 5)),
            dma((STEPS, chunks, spots - 1, 2, 3)),
            dma((STEPS, chunks, blks)),
            dma((STEPS, chunks, rows - 1)),
            dma((STEPS, chunks, rows - 1)),
            dma((STEPS, chunks, rows - 1)),
            dma((STEPS, chunks, rows - 1)),
            dma((STEPS, chunks, blks - 1)),
            dma((STEPS, chunks, blks - 1)),
        ],
        compiler_params=pltpu.CompilerParams(collective_id=0, has_side_effects=True),
    )(
        elastic_kernel.reshape(elastic_kernel.shape[1], elastic_kernel.shape[3]),
        slip_deficit.reshape(elements, members),
        state_variable.reshape(elements, members),
        step_size.reshape(1, members),
        load_stress.reshape(1, elements),
        normal_stress.reshape(1, elements),
        rate_table,
        evolve_table,
        patch_region.reshape(1, elements),
        creep_flag.reshape(1, elements),
    )
    return (
        velocity.reshape(slip_deficit.shape),
        deficit.reshape(slip_deficit.shape),
        state.reshape(slip_deficit.shape),
        step_next.reshape(members),
    )


def solution(mesh):
    placed = (
        P("blk", None, "row", None),
        P("blk", "row", None, None),
        P("blk", "row", None, None),
        P(),
        P("blk", "row", None),
        P("blk", "row", None),
        P(),
        P(),
        P("blk", "row", None),
        P("blk", "row", None),
    )
    return jax.shard_map(
        functools.partial(shards, mesh.shape["row"], mesh.shape["blk"]),
        mesh=mesh,
        in_specs=placed,
        out_specs=(
            P("blk", "row", None, None),
            P("blk", "row", None, None),
            P("blk", "row", None, None),
            P(),
        ),
        check_vma=False,
    )
```

```python
import functools

import jax
import jax.numpy as jnp
from jax import lax
from jax.experimental import pallas as pl
from jax.experimental.pallas import tpu as pltpu
from jax.sharding import PartitionSpec as P

NEWTON = 3
STEPS = 2
CORES = 2
CHUNK = 128
REACH = 2
EARLY = True

DAMPING = 0.5
PLATE_RATE = 1.0
STEP_CAP = 0.5

MESH = pl.DeviceIdType.MESH


def solve_rate(stress, factor, strength, creeping):
    slope = strength * factor
    speed = stress / (slope + DAMPING)
    for repeat in range(NEWTON):
        scaled = factor * speed
        size = jnp.abs(scaled)
        root = jnp.sqrt(size * size + 1.0)
        bend = jnp.log(size + root)
        bend = jnp.where(scaled < 0.0, -bend, bend)
        mismatch = strength * bend + DAMPING * speed - stress
        gradient = slope / root + DAMPING
        speed = speed - mismatch / gradient
    return jnp.where(creeping, jnp.float32(PLATE_RATE), speed)


def fault_kernel(
    rows,
    blks,
    chunks,
    elastic_in,
    deficit_in,
    state_in,
    step_ref,
    load_ref,
    normal_ref,
    rate_ref,
    evolve_ref,
    region_ref,
    creep_ref,
    velocity_out,
    deficit_out,
    state_out,
    next_out,
    tile,
    deficit,
    state,
    velocity,
    gathered,
    parts,
    own,
    partial,
    received,
    coefs,
    max_one,
    max_row,
    max_two,
    max_blk,
    load_sems,
    out_sems,
    own_sems,
    partner_sems,
    relay_sems,
    slip_sems,
    mirror_sems,
    sum_send,
    sum_recv,
    row_send,
    row_recv,
    blk_send,
    blk_recv,
):
    me_row = lax.axis_index("row")
    me_blk = lax.axis_index("blk")
    spots = blks // CORES
    spot = me_blk // CORES
    core = me_blk % CORES
    elements, width = deficit.shape[1:]
    half = elements // 2
    sent = []

    def columns(c):
        return pl.ds(c * width, width)

    def remote(src, dst, send_sem, recv_sem, row, blk):
        return pltpu.make_async_remote_copy(
            src_ref=src,
            dst_ref=dst,
            send_sem=send_sem,
            recv_sem=recv_sem,
            device_id={"row": row, "blk": blk},
            device_id_type=MESH,
        )

    def launch(copy, when=None):
        if when is None:
            copy.start()
        else:
            pl.when(when)(copy.start)
            sent.append((copy, when))

    def finished(place, sem):
        pltpu.make_async_copy(place, place, sem).wait()

    deficit_loads = [
        pltpu.make_async_copy(deficit_in.at[:, columns(c)], deficit.at[c], load_sems.at[0, c])
        for c in range(chunks)
    ]
    state_loads = [
        pltpu.make_async_copy(state_in.at[:, columns(c)], state.at[c], load_sems.at[1, c])
        for c in range(chunks)
    ]
    tile_load = pltpu.make_async_copy(elastic_in, tile, load_sems.at[2, 0])
    for copy in deficit_loads + state_loads + [tile_load]:
        copy.start()

    barrier = pltpu.get_barrier_semaphore()
    for j in range(1, rows):
        pl.semaphore_signal(
            barrier,
            inc=1,
            device_id={"row": lax.rem(me_row + j, rows), "blk": me_blk},
            device_id_type=MESH,
        )
    for j in range(1, blks):
        pl.semaphore_signal(
            barrier,
            inc=1,
            device_id={"row": me_row, "blk": lax.rem(me_blk + j, blks)},
            device_id_type=MESH,
        )
    for c in range(chunks):
        deficit_loads[c].wait()
        gathered[0, c, me_blk] = deficit[c].astype(jnp.bfloat16)
    pl.semaphore_wait(barrier, rows + blks - 2)

    reach = min(REACH, spots - 1)

    def slip_copy(t, c, block, target, send_sem, recv_sem):
        place = gathered.at[t, c, block]
        return remote(place, place, send_sem, recv_sem, me_row, target)

    def mirror(t, c, block, when=None):
        copy = slip_copy(
            t,
            c,
            block,
            spot * CORES + 1 - core,
            partner_sems.at[t, c],
            mirror_sems.at[t, c],
        )
        if when is None:
            copy.start()
        else:
            pl.when(when)(copy.start)

    def send_own(t, c):
        for i in range(reach, 0, -1):
            for j, shift in enumerate((i, -i)):
                target = spot + shift
                launch(
                    slip_copy(
                        t,
                        c,
                        me_blk,
                        target * CORES + core,
                        own_sems.at[t, c, i - 1, j],
                        slip_sems.at[t, c, spot],
                    ),
                    (target >= 0) & (target < spots),
                )
        mirror(t, c, me_blk)

    def collect(t, c, distances):
        for d in distances:
            for i, side in enumerate((-1, 1)):
                source = spot + side * d
                inside = (source >= 0) & (source < spots)
                block = source * CORES + core

                @pl.when(inside)
                def _():
                    finished(gathered.at[t, c, block], slip_sems.at[t, c, source])

                if d % reach == 0:
                    for shift in range(min(reach, spots - 1 - d), 0, -1):
                        target = spot - side * shift
                        launch(
                            slip_copy(
                                t,
                                c,
                                block,
                                target * CORES + core,
                                relay_sems.at[t, c, d - 1, i, shift - 1],
                                slip_sems.at[t, c, source],
                            ),
                            inside & (target >= 0) & (target < spots),
                        )
                mirror(t, c, block, inside)

    relayed = [d for d in range(reach, spots, reach) if d < spots - 1]
    others = [d for d in range(1, spots) if d not in relayed]

    def gather(t, c):
        collect(t, c, others)
        finished(gathered.at[t, c, :spots], mirror_sems.at[t, c])
        total = jnp.dot(
            tile[...],
            gathered[t, c].reshape(blks * elements, width),
            preferred_element_type=jnp.float32,
        ).reshape(rows, elements, width)
        parts[...] = total
        partial[t, c] = total.astype(jnp.bfloat16)
        for j in range(1, rows):
            target = lax.rem(me_row + j, rows)
            launch(
                remote(
                    partial.at[t, c, target],
                    received.at[t, c, j - 1],
                    sum_send.at[t, c],
                    sum_recv.at[t, c],
                    target,
                    me_blk,
                )
            )
        own[c] = parts[me_row]

    def first_round(t, c, largest):
        max_one[t, c] = largest
        for j in range(1, rows):
            launch(
                remote(
                    max_one.at[t, c],
                    max_row.at[t, c, j - 1],
                    row_send.at[t, c],
                    row_recv.at[t, c],
                    lax.rem(me_row + j, rows),
                    me_blk,
                )
            )

    def second_round(t, c):
        largest = max_one[t, c]
        finished(max_row.at[t, c], row_recv.at[t, c])
        for j in range(rows - 1):
            largest = jnp.maximum(largest, max_row[t, c, j])
        max_two[t, c] = largest
        for j in range(1, blks):
            launch(
                remote(
                    max_two.at[t, c],
                    max_blk.at[t, c, j - 1],
                    blk_send.at[t, c],
                    blk_recv.at[t, c],
                    me_row,
                    lax.rem(me_blk + j, blks),
                )
            )

    def next_step(t, c):
        largest = max_two[t, c]
        finished(max_blk.at[t, c], blk_recv.at[t, c])
        for j in range(blks - 1):
            largest = jnp.maximum(largest, max_blk[t, c, j])
        return STEP_CAP / (1.0 + largest)

    def friction(t, c):
        for h in range(2):
            part = pl.ds(h * half, half)
            coefs[4 + t, c, part] = 0.5 * jnp.exp(jnp.log(state[c, part]) * coefs[2, 0, part])

    def update(t, c):
        finished(received.at[t, c], sum_recv.at[t, c])
        last = t == STEPS - 1
        largest = jnp.zeros((1, width), jnp.float32)
        for h in range(2):
            part = pl.ds(h * half, half)
            stress = coefs[0, 0, part] + own[c, part]
            for j in range(rows - 1):
                stress = stress + received[t, c, j, part].astype(jnp.float32)
            speed = solve_rate(stress, coefs[4 + t, c, part], coefs[1, 0, part], coefs[3, 0, part] > 0.5)
            velocity[c, part] = speed
            largest = jnp.maximum(largest, jnp.max(jnp.abs(speed), axis=0, keepdims=True))
            if not last:
                moved = deficit[c, part] + step_ref[:, columns(c)] * (speed - PLATE_RATE)
                deficit[c, part] = moved
                gathered[t + 1, c, me_blk, part] = moved.astype(jnp.bfloat16)
        if last:
            first_round(t, c, largest)
            velocity_stores[c].start()
            step_now = next_step(t - 1, c)
        else:
            send_own(t + 1, c)
            first_round(t, c, largest)
            step_now = step_ref[:, columns(c)]
        for h in range(2):
            part = pl.ds(h * half, half)
            speed = velocity[c, part]
            old = state[c, part]
            state[c, part] = old * jnp.exp(step_now * (1.0 / old - jnp.abs(speed)))
            if last:
                deficit[c, part] = deficit[c, part] + step_now * (speed - PLATE_RATE)
        if last:
            deficit_stores[c].start()
            state_stores[c].start()
        else:
            friction(t + 1, c)

    velocity_stores, deficit_stores, state_stores = (
        [
            pltpu.make_async_copy(held.at[c], out.at[:, columns(c)], out_sems.at[i, c])
            for c in range(chunks)
        ]
        for i, (held, out) in enumerate(
            ((velocity, velocity_out), (deficit, deficit_out), (state, state_out))
        )
    )

    for c in range(chunks):
        send_own(0, c)

    region = region_ref[...]
    rate_coef = jnp.zeros(region.shape, jnp.float32)
    state_coef = jnp.zeros(region.shape, jnp.float32)
    for level in range(rate_ref.shape[0]):
        match = region == level
        rate_coef = jnp.where(match, rate_ref[level], rate_coef)
        state_coef = jnp.where(match, evolve_ref[level], state_coef)

    def spread(line):
        return jnp.transpose(jnp.broadcast_to(line, (width, elements)))

    coefs[0, 0] = spread(load_ref[...])
    coefs[1, 0] = spread(normal_ref[...] * rate_coef)
    coefs[2, 0] = spread(state_coef / rate_coef)
    coefs[3, 0] = spread(jnp.where(creep_ref[...] == 1, 1.0, 0.0))
    for c in range(chunks):
        state_loads[c].wait()
        friction(0, c)
    tile_load.wait()

    def drain(t, c):
        finished(gathered.at[t, c, :spots], partner_sems.at[t, c])
        finished(received.at[t, c], sum_send.at[t, c])

    def drain_slips():
        for copy, when in sent:
            pl.when(when)(copy.wait_send)

    lag = 1 if chunks > 1 else 0
    ahead = 1 if EARLY and chunks > 2 else 0
    stages = [(t, c) for t in range(STEPS) for c in range(chunks)]
    total = len(stages)
    for s in range(ahead):
        collect(*stages[s], relayed)
    for s in range(total + lag + 1):
        if not ahead and s < total:
            collect(*stages[s], relayed)
        if s < total:
            gather(*stages[s])
        if ahead and s + ahead < total:
            collect(*stages[s + ahead], relayed)
        if 0 <= s - lag < total:
            update(*stages[s - lag])
        if s == total + lag - 1:
            for stage in stages:
                drain(*stage)
            drain_slips()
        if 0 <= s - lag - 1 < total:
            second_round(*stages[s - lag - 1])
    for copy in velocity_stores + deficit_stores + state_stores:
        copy.wait()
    for t, c in stages:
        finished(max_row.at[t, c], row_send.at[t, c])
        finished(max_blk.at[t, c], blk_send.at[t, c])
    for c in range(chunks):
        next_out[:, columns(c)] = next_step(STEPS - 1, c)


def hand_over(velocity_in, deficit_in, state_in, next_in, velocity_out, deficit_out, state_out, next_out, held, sems):
    pairs = ((velocity_in, velocity_out), (deficit_in, deficit_out), (state_in, state_out))
    loads = [pltpu.make_async_copy(pair[0], held.at[i], sems.at[0, i]) for i, pair in enumerate(pairs)]
    stores = [pltpu.make_async_copy(held.at[i], pair[1], sems.at[1, i]) for i, pair in enumerate(pairs)]
    for copy in loads:
        copy.start()
    next_out[...] = next_in[...]
    for load, store in zip(loads, stores):
        load.wait()
        store.start()
    for copy in stores:
        copy.wait()


def shards(
    rows,
    blks,
    elastic_kernel,
    slip_deficit,
    state_variable,
    step_size,
    load_stress,
    normal_stress,
    rate_table,
    evolve_table,
    patch_region,
    creep_flag,
):
    elements, members = slip_deficit.shape[2:]
    width = CHUNK if members % CHUNK == 0 else members
    chunks = members // width
    spots = blks // CORES
    reach = min(REACH, spots - 1)
    anywhere = pl.BlockSpec(memory_space=pl.ANY)
    vmem = pl.BlockSpec(memory_space=pltpu.VMEM)
    smem = pl.BlockSpec(memory_space=pltpu.SMEM)
    block = jax.ShapeDtypeStruct((elements, members), jnp.float32)
    dma = pltpu.SemaphoreType.DMA
    solved = pl.pallas_call(
        functools.partial(fault_kernel, rows, blks, chunks),
        out_shape=(block, block, block, jax.ShapeDtypeStruct((1, members), jnp.float32)),
        in_specs=[anywhere] * 3 + [vmem] * 3 + [smem] * 2 + [vmem] * 2,
        out_specs=(anywhere, anywhere, anywhere, vmem),
        scratch_shapes=[
            pltpu.VMEM((elastic_kernel.shape[1], elastic_kernel.shape[3]), jnp.bfloat16),
            pltpu.VMEM((chunks, elements, width), jnp.float32),
            pltpu.VMEM((chunks, elements, width), jnp.float32),
            pltpu.VMEM((chunks, elements, width), jnp.float32),
            pltpu.VMEM((STEPS, chunks, blks, elements, width), jnp.bfloat16),
            pltpu.VMEM((rows, elements, width), jnp.float32),
            pltpu.VMEM((chunks, elements, width), jnp.float32),
            pltpu.VMEM((STEPS, chunks, rows, elements, width), jnp.bfloat16),
            pltpu.VMEM((STEPS, chunks, rows - 1, elements, width), jnp.bfloat16),
            pltpu.VMEM((4 + STEPS, chunks, elements, width), jnp.float32),
            pltpu.VMEM((STEPS, chunks, 1, width), jnp.float32),
            pltpu.VMEM((STEPS, chunks, rows - 1, 1, width), jnp.float32),
            pltpu.VMEM((STEPS, chunks, 1, width), jnp.float32),
            pltpu.VMEM((STEPS, chunks, blks - 1, 1, width), jnp.float32),
            dma((3, chunks)),
            dma((3, chunks)),
            dma((STEPS, chunks, reach, 2)),
            dma((STEPS, chunks)),
            dma((STEPS, chunks, spots - 1, 2, reach)),
            dma((STEPS, chunks, spots)),
            dma((STEPS, chunks)),
            dma((STEPS, chunks)),
            dma((STEPS, chunks)),
            dma((STEPS, chunks)),
            dma((STEPS, chunks)),
            dma((STEPS, chunks)),
            dma((STEPS, chunks)),
        ],
        compiler_params=pltpu.CompilerParams(collective_id=0, has_side_effects=True),
    )(
        elastic_kernel.reshape(elastic_kernel.shape[1], elastic_kernel.shape[3]),
        slip_deficit.reshape(elements, members),
        state_variable.reshape(elements, members),
        step_size.reshape(1, members),
        load_stress.reshape(1, elements),
        normal_stress.reshape(1, elements),
        rate_table,
        evolve_table,
        patch_region.reshape(1, elements),
        creep_flag.reshape(1, elements),
    )
    velocity, deficit, state, step_next = pl.pallas_call(
        hand_over,
        out_shape=(block, block, block, jax.ShapeDtypeStruct((1, members), jnp.float32)),
        in_specs=[anywhere] * 3 + [vmem],
        out_specs=(anywhere, anywhere, anywhere, vmem),
        scratch_shapes=[pltpu.VMEM((3, elements, members), jnp.float32), dma((2, 3))],
    )(*solved)
    return (
        velocity.reshape(slip_deficit.shape),
        deficit.reshape(slip_deficit.shape),
        state.reshape(slip_deficit.shape),
        step_next.reshape(members),
    )


def solution(mesh):
    placed = (
        P("blk", None, "row", None),
        P("blk", "row", None, None),
        P("blk", "row", None, None),
        P(),
        P("blk", "row", None),
        P("blk", "row", None),
        P(),
        P(),
        P("blk", "row", None),
        P("blk", "row", None),
    )
    return jax.shard_map(
        functools.partial(shards, mesh.shape["row"], mesh.shape["blk"]),
        mesh=mesh,
        in_specs=placed,
        out_specs=(
            P("blk", "row", None, None),
            P("blk", "row", None, None),
            P("blk", "row", None, None),
            P(),
        ),
        check_vma=False,
    )
```
